8 devices in a mesh: ty: 2 (over z, y), tx: 4 (over x, core).
Axes of the slice: x: 2, y: 2, z: 1, core: 2. Of those that a mesh axis runs over, the one named last changes fastest.
Arguments:
- w_in: float32 [4, 2, 6, 256, 1024], P('tx', 'ty')
- w_out: float32 [4, 2, 6, 1024, 256], P('tx', 'ty')
- inputs: bfloat16 [4, 2, 7, 4096, 256], P('tx', 'ty')
- targets: bfloat16 [4, 2, 7, 4096, 256], P('tx', 'ty')
Outputs:
- output 1: float32 [4, 2, 6, 256, 1024], P('tx', 'ty')
- output 2: float32 [4, 2, 6, 1024, 256], P('tx', 'ty')
- output 3: float32 [4, 2, 6, 256, 1024], P('tx', 'ty')
- output 4: float32 [4, 2, 6, 1024, 256], P('tx', 'ty')
All inputs are finite; a program needn't handle non-finite values.
Results may differ from the reference program's by a relative error of at most 0.00551442.
Values are sent between devices in bfloat16 or wider.
A program may use at most 1 GiB of HBM per device.

```python
import jax
import jax.numpy as jnp
from jax import lax

TX = 4
TY = 2
LAYERS = 6
D = 256
FF = 1024
ROWS = 4096
STEPS = 6
EPS = 1e-6
LEARN_RATE = 0.125


def setup_inputs(seed: int = 0) -> dict:
    root_key = jax.random.key(seed)
    key_list = jax.random.split(root_key, 6)
    base_in = jax.random.normal(key_list[0], (LAYERS, D, FF), jnp.float32)
    own_in = jax.random.normal(key_list[1], (TX, TY, LAYERS, D, FF), jnp.float32)
    w_in = (base_in[None, None] + 0.5 * own_in) * (D ** -0.5)
    base_out = jax.random.normal(key_list[2], (LAYERS, FF, D), jnp.float32)
    own_out = jax.random.normal(key_list[3], (TX, TY, LAYERS, FF, D), jnp.float32)
    w_out = (base_out[None, None] + 0.5 * own_out) * (FF ** -0.5)
    inputs = jax.random.normal(key_list[4], (TX, TY, STEPS + 1, ROWS, D), jnp.float32).astype(jnp.bfloat16)
    targets = jax.random.normal(key_list[5], (TX, TY, STEPS + 1, ROWS, D), jnp.float32).astype(jnp.bfloat16)
    return {'w_in': w_in, 'w_out': w_out, 'inputs': inputs, 'targets': targets}


def layer_step(hidden, weights):
    mat_in, mat_out = weights
    hidden_f32 = hidden.astype(jnp.float32)
    inv_rms = lax.rsqrt(jnp.mean(hidden_f32 * hidden_f32, axis=-1, keepdims=True) + EPS)
    normed = (hidden_f32 * inv_rms).astype(jnp.bfloat16)
    pre_act = jnp.dot(normed, mat_in.astype(jnp.bfloat16), preferred_element_type=jnp.float32)
    gelu_out = jax.nn.gelu(pre_act).astype(jnp.bfloat16)
    mlp_out = jnp.dot(gelu_out, mat_out.astype(jnp.bfloat16), preferred_element_type=jnp.float32)
    return (hidden_f32 + mlp_out).astype(jnp.bfloat16), None


def local_loss(w_in, w_out, batch_in, batch_tgt):
    last_hidden, _ = lax.scan(layer_step, batch_in, (w_in, w_out))
    resid_err = last_hidden.astype(jnp.float32) - batch_tgt.astype(jnp.float32)
    return jnp.mean(resid_err * resid_err)


local_grads = jax.grad(local_loss, argnums=(0, 1))


def gossip_mix(values):
    sent_copy = values.astype(jnp.bfloat16).astype(jnp.float32)
    summed = values + jnp.roll(sent_copy, 1, axis=0)
    summed = summed + jnp.roll(sent_copy, -1, axis=0)
    summed = summed + jnp.roll(sent_copy, 1, axis=1)
    summed = summed + jnp.roll(sent_copy, -1, axis=1)
    return summed / 5.0


def reference(w_in, w_out, inputs, targets):
    cell_count = TX * TY
    step_size = LEARN_RATE

    def one_cell(operands):
        return local_grads(operands[0], operands[1], operands[2], operands[3])

    def all_grads(p_in, p_out, step_idx):
        batch_in = lax.dynamic_index_in_dim(inputs, step_idx, axis=2, keepdims=False).reshape((cell_count, ROWS, D))
        batch_tgt = lax.dynamic_index_in_dim(targets, step_idx, axis=2, keepdims=False).reshape((cell_count, ROWS, D))
        grad_in, grad_out = lax.map(one_cell, (p_in.reshape((cell_count, LAYERS, D, FF)), p_out.reshape((cell_count, LAYERS, FF, D)), batch_in, batch_tgt))
        return grad_in.reshape(p_in.shape), grad_out.reshape(p_out.shape)

    first_in, first_out = all_grads(w_in, w_out, 0)

    def step_body(carried, step_idx):
        p_in, p_out, y_in, y_out, old_in, old_out = carried
        p_in = gossip_mix(p_in) - step_size * y_in
        p_out = gossip_mix(p_out) - step_size * y_out
        new_gin, new_gout = all_grads(p_in, p_out, step_idx)
        y_in = gossip_mix(y_in) + new_gin - old_in
        y_out = gossip_mix(y_out) + new_gout - old_out
        return (p_in, p_out, y_in, y_out, new_gin, new_gout), None

    final_state, _ = lax.scan(step_body, (w_in, w_out, first_in, first_out, first_in, first_out), jnp.arange(1, STEPS + 1))
    return (final_state[0], final_state[1], final_state[2], final_state[3])
```

```python
import functools
import math

import jax
import jax.numpy as jnp
from jax import lax
from jax.experimental import pallas as pl
from jax.experimental.pallas import tpu as pltpu
from jax.sharding import PartitionSpec as P

EPS = 1e-6
LEARN_RATE = 0.125
C0 = math.sqrt(2.0 / math.pi)
C1 = C0 * 0.044715
BF16 = jnp.bfloat16
F32 = jnp.float32


def _dot(lhs, rhs, lhs_dim=1, rhs_dim=0):
    return lax.dot_general(
        lhs, rhs, (((lhs_dim,), (rhs_dim,)), ((), ())), preferred_element_type=F32
    )


def grad_kernel(layers, d, ff, rb, nb, fc, *refs):
    msg = refs[:layers]
    x_ref, t_ref = refs[layers:layers + 2]
    g_out = refs[layers + 2:2 * layers + 2]
    w_s, acc_s, h_s, ut_s, inv_s, a_s, gp_s, in_sem, out_sem = refs[2 * layers + 2:]
    step = pl.program_id(0)
    chunks = [pl.ds(c * fc, fc) for c in range(ff // fc)]
    top = pl.ds(0, d)
    low = pl.ds(d, d)

    @pl.when(step == 0)
    def _():
        copies = [
            pltpu.make_async_copy(msg[l].at[pl.ds(0, 2 * d)], w_s.at[l], in_sem.at[l])
            for l in range(layers)
        ]
        for copy in copies:
            copy.start()

        def clear(l, carry):
            acc_s[l] = jnp.zeros_like(acc_s[l])
            return carry

        lax.fori_loop(0, layers, clear, 0)
        for copy in copies:
            copy.wait()

    h_s[0] = x_ref[...]

    def forward(l, carry):
        hf = h_s[l].astype(F32)
        inv = lax.rsqrt(jnp.mean(hf * hf, axis=-1, keepdims=True) + EPS)
        inv_s[l] = inv
        u = (hf * inv).astype(BF16)
        ut_s[l] = u.T
        out = hf
        for cs in chunks:
            z = _dot(u, w_s[l, top, cs])
            z2 = z * z
            s = 0.5 * jnp.tanh(z * (C0 + C1 * z2)) + 0.5
            a = z * s
            a_s[l, :, cs] = a.astype(BF16)
            gp_s[l, :, cs] = s + (a * (1.0 - s)) * (2.0 * C0 + (6.0 * C1) * z2)
        out = hf + _dot(a_s[l], w_s[l, low, :], 1, 1)
        h_s[l + 1] = out.astype(BF16)
        return carry

    lax.fori_loop(0, layers, forward, 0)

    err = h_s[layers].astype(F32) - t_ref[...].astype(F32)
    h_s[layers] = (err * (2.0 / (rb * nb * d))).astype(BF16)

    def backward(l, with_input):
        dh = h_s[l + 1]
        dht = dh.T
        ut = ut_s[l]
        for cs in chunks:
            da = _dot(dh, w_s[l, low, cs]).astype(BF16).astype(F32)
            dz = (da * gp_s[l, :, cs]).astype(BF16)
            acc_s[l, low, cs] += _dot(dht, a_s[l, :, cs])
            a_s[l, :, cs] = dz
            acc_s[l, top, cs] += _dot(ut, dz)
        if with_input:
            dn = _dot(a_s[l], w_s[l, top, :], 1, 1).astype(BF16).astype(F32)
            hf = h_s[l].astype(F32)
            inv = inv_s[l]
            coef = (inv * inv * inv * (1.0 / d)) * jnp.sum(dn * hf, axis=-1, keepdims=True)
            h_s[l] = (dh.astype(F32) + dn * inv - hf * coef).astype(BF16)

    def backward_body(k, carry):
        backward(layers - 1 - k, True)
        return carry

    lax.fori_loop(0, layers - 1, backward_body, 0)
    backward(0, False)

    @pl.when(step == nb - 1)
    def _():
        def narrow(l, carry):
            w_s[l] = acc_s[l].astype(BF16)
            return carry

        lax.fori_loop(0, layers, narrow, 0)
        copies = [pltpu.make_async_copy(w_s.at[l], g_out[l], out_sem.at[l]) for l in range(layers)]
        for copy in copies:
            copy.start()
        for copy in copies:
            copy.wait()


def make_grad(layers, d, ff, rows, rb=512, fc=256):
    nb = rows // rb

    def call(msgs, inputs, targets, batch):
        batch_spec = pl.BlockSpec((None, None, None, rb, d), lambda i: (0, 0, batch, i, 0))
        any_spec = pl.BlockSpec(memory_space=pl.ANY)
        mm = 2 * rows * d * ff * layers
        return pl.pallas_call(
            functools.partial(grad_kernel, layers, d, ff, rb, nb, fc),
            grid=(nb,),
            in_specs=[any_spec] * layers + [batch_spec, batch_spec],
            out_specs=[any_spec] * layers,
            out_shape=[jax.ShapeDtypeStruct((2 * d, ff), BF16)] * layers,
            scratch_shapes=[
                pltpu.VMEM((layers, 2 * d, ff), BF16),
                pltpu.VMEM((layers, 2 * d, ff), F32),
                pltpu.VMEM((layers + 1, rb, d), BF16),
                pltpu.VMEM((layers, d, rb), BF16),
                pltpu.VMEM((layers, rb, 1), F32),
                pltpu.VMEM((layers, rb, ff), BF16),
                pltpu.VMEM((layers, rb, ff), F32),
                pltpu.SemaphoreType.DMA((layers,)),
                pltpu.SemaphoreType.DMA((layers,)),
            ],
            compiler_params=pltpu.CompilerParams(
                dimension_semantics=("arbitrary",), vmem_limit_bytes=60 * 1024 * 1024
            ),
            cost_estimate=pl.CostEstimate(
                flops=6 * mm, bytes_accessed=rows * d * 4 + layers * 8 * d * ff, transcendentals=rows * ff * layers
            ),
            name="grad",
        )(*msgs, inputs, targets)

    return call


def mix_kernel(d2, has_y, want_p_msg, want_p, *refs):
    it = iter(refs)
    p_ref = next(it) if want_p else None
    y_ref = next(it) if has_y else None
    nbr = [next(it) for _ in range(3)]
    g_ref = next(it)
    gold_ref = next(it) if has_y else None
    p_out = next(it) if want_p else None
    y_out = next(it)
    m_out = next(it) if want_p else None

    def mix(own, idx):
        xm, xp, yy = [r[idx].astype(F32) for r in nbr]
        return (own + xm + xp + yy + yy) / 5.0

    g = g_ref[...].astype(F32)
    y = (mix(y_ref[...], 1 if want_p else 0) + g) - gold_ref[...].astype(F32) if has_y else g
    y_out[...] = y
    if want_p:
        p = mix(p_ref[...], 0) - LEARN_RATE * y
        p_out[...] = p
        m_out[0] = p.astype(BF16)
        m_out[1] = y.astype(BF16)


def mix_call(p, y, nbrs, g, g_old, want_p=True, rows_blk=128):
    has_y = y is not None
    d2, ff = g.shape
    nm = nbrs[0].shape[0]
    blk = pl.BlockSpec((rows_blk, ff), lambda i: (i, 0))
    mblk = pl.BlockSpec((nm, rows_blk, ff), lambda i: (0, i, 0))
    oblk = pl.BlockSpec((2, rows_blk, ff), lambda i: (0, i, 0))
    args, specs = [], []
    if want_p:
        args.append(p)
        specs.append(blk)
    if has_y:
        args.append(y)
        specs.append(blk)
    args += list(nbrs) + [g]
    specs += [mblk] * 3 + [blk]
    if has_y:
        args.append(g_old)
        specs.append(blk)
    st = jax.ShapeDtypeStruct((d2, ff), F32)
    outs = ([st] if want_p else []) + [st]
    ospecs = ([blk] if want_p else []) + [blk]
    if want_p:
        outs.append(jax.ShapeDtypeStruct((2, d2, ff), BF16))
        ospecs.append(oblk)
    n = d2 * ff
    res = pl.pallas_call(
        functools.partial(mix_kernel, d2, has_y, want_p, want_p),
        grid=(d2 // rows_blk,),
        in_specs=specs,
        out_specs=ospecs,
        out_shape=outs,
        compiler_params=pltpu.CompilerParams(dimension_semantics=("arbitrary",)),
        cost_estimate=pl.CostEstimate(flops=20 * n, bytes_accessed=36 * n, transcendentals=0),
        name="mix",
    )(*args)
    return res if want_p else (None, res[0], None)


def solution(mesh):
    size_x = mesh.shape['tx']
    size_y = mesh.shape['ty']

    def shift(values, axis_name, axis_size, offset):
        return lax.ppermute(values, axis_name, [(s, (s + offset) % axis_size) for s in range(axis_size)])

    def exchange(msg):
        return (
            shift(msg, 'tx', size_x, 1),
            shift(msg, 'tx', size_x, -1),
            shift(msg, 'ty', size_y, 1),
        )

    def device_fn(w_in, w_out, inputs, targets):
        layers, d, ff = w_in.shape[2:]
        steps, rows = inputs.shape[2] - 1, inputs.shape[3]
        grad = make_grad(layers, d, ff, rows)
        p = [jnp.concatenate([w_in[0, 0, l], w_out[0, 0, l].T], axis=0) for l in range(layers)]
        msg = [v.astype(BF16)[None] for v in p]
        y = [None] * layers
        g_old = [None] * layers
        for t in range(steps + 1):
            last = t == steps
            got = [exchange(m if t < steps else m[1:]) for m in msg]
            g = grad([m.reshape(-1, ff) for m in msg], inputs, targets, t)
            for l in range(layers):
                new_p, y[l], msg[l] = mix_call(p[l], y[l], got[l], g[l], g_old[l], want_p=not last)
                if not last:
                    p[l] = new_p
            g_old = g
        p_in = jnp.stack([v[:d] for v in p])
        p_out = jnp.stack([v[d:].T for v in p])
        y_in = jnp.stack([v[:d] for v in y])
        y_out = jnp.stack([v[d:].T for v in y])
        return p_in[None, None], p_out[None, None], y_in[None, None], y_out[None, None]

    block_spec = P('tx', 'ty')
    return jax.shard_map(device_fn, mesh=mesh, in_specs=(block_spec,) * 4, out_specs=(block_spec,) * 4, check_vma=False)
```
